128 devices in a mesh: tm: 2 (over z_lo), grid: 64 (over z_hi, y, x, core).
Axes of the slice: x: 4, y: 4, z: 4 (z_hi: 2, z_lo: 2; z = z_hi * 2 + z_lo), core: 2. Of those that a mesh axis runs over, the one named last changes fastest.
Arguments:
- occupied_green: bfloat16 [2, 1024, 1024], P('tm', 'grid'), may hold values from -0.005859375 to 0.005859375
- empty_green: bfloat16 [2, 1024, 1024], P('tm', 'grid'), may hold values from -0.005859375 to 0.005859375
- basis: bfloat16 [12288, 1024], P('grid'), may hold values from -8 to 8
- time_weights: float32 [2, 2], replicated, may hold values from 0.25 to 1
Outputs:
- polarizability: float32 [2, 1024, 1024], P('tm', 'grid')
The draws below stay inside these ranges and needn't reach their ends.
All inputs are finite; a program needn't handle non-finite values.
Results may differ from the reference program's by a relative error of at most 0.0012.
Values may be sent and summed in bfloat16 or wider, within the bound.
No kernel may reach another device: no remote copies, remote signals or barrier semaphores. Data moves between devices by JAX's collectives and lax.ppermute only.
A program may use at most 128 MiB of HBM per device.

```python
import math
import jax
import jax.numpy as jnp
from jax import lax

NR = 12288
NB = 1024
TIMES = 2
FREQS = 2


def draw_basis(key, part):
    draw_keys = jax.random.split(jax.random.fold_in(key, 7103), 5)
    positions = jnp.arange(NR, dtype=jnp.float32)[:, None]
    centres = jax.random.uniform(draw_keys[0], (1, NB), jnp.float32, 0.0, float(NR))
    spreads = jnp.exp(jax.random.uniform(draw_keys[1], (1, NB), jnp.float32, math.log(2.0 * NR / NB), math.log(NR / 8.0)))
    offsets = jnp.abs(positions - centres)
    distance = jnp.minimum(offsets, float(NR) - offsets)
    wavenumber = jax.random.uniform(draw_keys[2], (1, NB), jnp.float32, 0.5, 3.0) * (2.0 * math.pi) / spreads
    phases = jax.random.uniform(draw_keys[3], (1, NB), jnp.float32, -math.pi, math.pi)
    relative = distance / spreads
    envelope = 0.2 + 1.0 / (1.0 + relative * relative)
    profile = envelope * jnp.cos(wavenumber * distance + phases)
    roughness = jax.random.uniform(draw_keys[4], (NR, NB), jnp.float32, 0.5, 1.5)
    unscaled = profile * roughness
    rms_value = jnp.sqrt(jnp.mean(unscaled * unscaled))
    return jnp.clip(unscaled / rms_value, -8.0, 8.0).astype(jnp.bfloat16)


def level_of(rng, extent, cuts, least, largest):
    def one(dim, blocks):
        steps = jax.random.uniform(jax.random.fold_in(jax.random.fold_in(rng, 6), dim), (blocks,), jnp.float32, least / len(cuts), largest / len(cuts))
        return jnp.repeat(jnp.exp(steps), extent[dim] // blocks).reshape((-1,) + (1,) * (len(extent) - dim - 1))

    factor_of = one(*cuts[0])
    for cut in cuts[1:]:
        factor_of = factor_of * one(*cut)
    return factor_of


def normal_values(key, shape, spread, limit, pieces=(), kind=jnp.bfloat16):
    entries = spread * jax.random.normal(key, shape, jnp.float32)
    if pieces:
        entries = entries * level_of(key, shape, pieces, -0.22, 0.18)
    return jnp.clip(entries, -limit, limit).astype(kind)


def setup_inputs(seed: int = 0) -> dict:
    streams_of = jax.random.split(jax.random.key(seed), 5)
    return {
        "occupied_green": normal_values(streams_of[0], (TIMES, NB, NB), (NB * NB) ** -0.5, 0.005859375, ((0, 2), (1, 64))),
        "empty_green": normal_values(streams_of[1], (TIMES, NB, NB), (NB * NB) ** -0.5, 0.005859375, ((0, 2), (1, 64))),
        "basis": draw_basis(jax.random.fold_in(streams_of[4], 71), 0),
        "time_weights": jnp.clip(jax.random.uniform(streams_of[3], (FREQS, TIMES), jnp.float32, 0.25, 1.0), 0.25, 1.0),
    }


def reference(occupied_green, empty_green, basis, time_weights):
    block_rows = math.gcd(NR, 2048)
    block_total = NR // block_rows
    scale_factor = 1.0 / NR
    totals = []
    for time_increment in range(TIMES):
        occupied_now = occupied_green[time_increment]
        empty_now = empty_green[time_increment]

        def one_block(block_index):
            local_rows = lax.dynamic_slice_in_dim(basis, block_index * block_rows, block_rows, 0)
            occ_proj = jnp.dot(local_rows, occupied_now.T, preferred_element_type=jnp.float32).astype(jnp.bfloat16)
            emp_proj = jnp.dot(local_rows, empty_now.T, preferred_element_type=jnp.float32).astype(jnp.bfloat16)
            occ_real = jnp.dot(occ_proj, basis.T, preferred_element_type=jnp.float32)
            emp_real = jnp.dot(emp_proj, basis.T, preferred_element_type=jnp.float32)
            product = (occ_real * emp_real).astype(jnp.bfloat16)
            back_half = jnp.dot(product, basis, preferred_element_type=jnp.float32).astype(jnp.bfloat16)
            return jnp.dot(back_half.T, local_rows, preferred_element_type=jnp.float32)

        partial_sets = lax.map(one_block, jnp.arange(block_total, dtype=jnp.int32))
        totals.append(jnp.sum(partial_sets, axis=0))
    result_list = []
    for freq_step in range(FREQS):
        accum = jnp.zeros((NB, NB), jnp.float32)
        for time_increment in range(TIMES):
            accum = accum + time_weights[freq_step, time_increment] * totals[time_increment]
        result_list.append(scale_factor * accum)
    return jnp.stack(result_list)
```

```python
import jax
import jax.numpy as jnp
from jax import lax
from jax.experimental import pallas as pl
from jax.experimental.pallas import tpu as pltpu
from jax.sharding import Mesh
from jax.sharding import PartitionSpec as P

NR = 12288
NB = 1024
GRID = ("zh", "y", "x", "core")
BF = jnp.bfloat16
F32 = jnp.float32
ANY = pl.BlockSpec(memory_space=pl.ANY)
MIB = 1024 * 1024


def shift(v, axis, step):
    n = lax.axis_size(axis)
    return lax.ppermute(v, axis, [(i, (i + step) % n) for i in range(n)])


def far_z(v):
    return lax.ppermute(v, ("tm", "zh"), [(0, 3), (3, 0), (1, 2), (2, 1)])


def after(v, *deps):
    return lax.optimization_barrier((v, *deps))[0]


def nt(a, b):
    return lax.dot_general(a, b, (((1,), (1,)), ((), ())), preferred_element_type=F32)


def copy_all(copies):
    for c in copies:
        c.start()
    for c in copies:
        c.wait()


def row_copies(pieces, dst, sems, first):
    out, row = [], 0
    for j, p in enumerate(pieces):
        rows = p.shape[0]
        out.append(pltpu.make_async_copy(p, dst.at[pl.ds(row, rows)], sems.at[first + j]))
        row += rows
    return out


S_PLAN = ((0, 0), (3, 0), (1, 0), (2, 0), (2, 96))


def project_kernel(n_s, green_plan, *refs):
    s_pieces = refs[:n_s]
    greens = refs[n_s : n_s + len(green_plan)]
    proj_ref, block_ref, green, sems = refs[n_s + len(green_plan) :]
    zh, y, x, core = (lax.axis_index(a) for a in GRID)
    copies = []
    for n, p in enumerate(s_pieces):
        dx, first = S_PLAN[n % len(S_PLAN)]
        cc = core if n < len(S_PLAN) else 1 - core
        row = pl.multiple_of((lax.rem(x + dx, 4) * 2 + cc) * 192 + first, 32)
        to = block_ref.at[pl.ds(row, p.shape[0])]
        copies.append(pltpu.make_async_copy(p, to, sems.at[n]))
    n = n_s
    for ref, (dx, other, dys) in zip(greens, green_plan):
        for j, dy in enumerate(dys):
            for h in range(2):
                zz = zh if h == 0 else 1 - zh
                cc = core if not other else 1 - core
                dev = ((zz * 4 + lax.rem(y + dy, 4)) * 4 + lax.rem(x + dx, 4)) * 2 + cc
                row = pl.multiple_of(dev * 16, 16)
                for q in range(2):
                    copies.append(
                        pltpu.make_async_copy(
                            ref.at[j, h, q], green.at[q, pl.ds(row, 16)], sems.at[n]
                        )
                    )
                    n += 1
    copy_all(copies)
    rows = 256

    def one(i, carry):
        at = pl.ds(pl.multiple_of(i * rows, rows), rows)
        for q in range(2):
            proj_ref[q, at] = nt(block_ref[at], green[q]).astype(BF)
        return carry

    lax.fori_loop(0, block_ref.shape[0] // rows, one, 0)


def project(s_pieces, greens, green_plan):
    rows = sum(p.shape[0] for p in s_pieces)
    n_copies = len(s_pieces) + sum(4 * len(p[2]) for p in green_plan)

    def kernel(*refs):
        project_kernel(len(s_pieces), green_plan, *refs)

    return pl.pallas_call(
        kernel,
        out_shape=(
            jax.ShapeDtypeStruct((2, rows, NB), BF),
            jax.ShapeDtypeStruct((rows, NB), BF),
        ),
        in_specs=[ANY] * (len(s_pieces) + len(greens)),
        out_specs=(
            pl.BlockSpec(memory_space=pltpu.VMEM),
            pl.BlockSpec(memory_space=pltpu.VMEM),
        ),
        scratch_shapes=[pltpu.VMEM((2, NB, NB), BF), pltpu.SemaphoreType.DMA((n_copies,))],
        compiler_params=pltpu.CompilerParams(vmem_limit_bytes=20 * MIB),
        cost_estimate=pl.CostEstimate(
            flops=4 * rows * NB * NB, bytes_accessed=14 * 2**20, transcendentals=0
        ),
        name="project",
    )(*s_pieces, *greens)


S_TILE = 512
R_TILE = 512
K_TILE = 256


def main_kernel(n_r, proj_ref, *refs):
    pieces = refs[:n_r]
    own_ref, other_ref, block, block_t, product, sems = refs[n_r:]
    core = lax.axis_index("core")
    r_rows = block.shape[0]

    @pl.when(pl.program_id(0) == 0)
    def _():
        copy_all(row_copies(pieces, block, sems, 0))

        def turn(i, carry):
            at = pl.ds(pl.multiple_of(i * 256, 256), 256)
            block_t[:, at] = block[at].T
            return carry

        lax.fori_loop(0, r_rows // 256, turn, 0)

    def real_space(i, carry):
        at = pl.ds(pl.multiple_of(i * R_TILE, R_TILE), R_TILE)
        rows = block[at]
        product[:, at] = (nt(proj_ref[0], rows) * nt(proj_ref[1], rows)).astype(BF)
        return carry

    lax.fori_loop(0, r_rows // R_TILE, real_space, 0)

    def back_half(i, carry):
        at = pl.ds(pl.multiple_of(i * K_TILE, K_TILE), K_TILE)
        back = nt(block_t[at], product[...]).astype(BF)
        groups = K_TILE // 32
        back = back.reshape(groups, 2, 16, back.shape[1])
        to = pl.ds(pl.multiple_of(i * groups, groups), groups)
        own_ref[to] = jnp.where(core == 0, back[:, 0], back[:, 1])
        other_ref[to] = jnp.where(core == 0, back[:, 1], back[:, 0])
        return carry

    lax.fori_loop(0, NB // K_TILE, back_half, 0)


def main(proj, pieces):
    s_rows = proj.shape[1]
    r_rows = sum(p.shape[0] for p in pieces)
    half = jax.ShapeDtypeStruct((NB // 32, 16, s_rows), BF)
    half_spec = pl.BlockSpec((NB // 32, 16, S_TILE), lambda i: (0, 0, i))

    def kernel(*refs):
        main_kernel(len(pieces), *refs)

    return pl.pallas_call(
        kernel,
        grid=(s_rows // S_TILE,),
        out_shape=(half, half),
        in_specs=[pl.BlockSpec((2, S_TILE, NB), lambda i: (0, i, 0))] + [ANY] * len(pieces),
        out_specs=(half_spec, half_spec),
        scratch_shapes=[
            pltpu.VMEM((r_rows, NB), BF),
            pltpu.VMEM((NB, r_rows), BF),
            pltpu.VMEM((S_TILE, r_rows), BF),
            pltpu.SemaphoreType.DMA((len(pieces),)),
        ],
        compiler_params=pltpu.CompilerParams(vmem_limit_bytes=28 * MIB),
        cost_estimate=pl.CostEstimate(
            flops=6 * s_rows * r_rows * NB, bytes_accessed=12 * MIB, transcendentals=0
        ),
        name="main",
    )(proj, *pieces)


def gather_points_x(b):
    xm, xp = shift(b, "x", 1), shift(b, "x", -1)
    half = b.shape[0] // 2
    far0 = shift(xm[:half], "x", 1)
    far1 = shift(xp[half:], "x", -1)
    mine = [b, xm, xp, far0, far1]
    return mine + [shift(v, "core", 1) for v in mine], (far0, far1)


def gather_points_yz(b, y_after):
    zb = far_z(b)
    by = after(b, *y_after)
    ym, yp = shift(by, "y", 1), shift(by, "y", -1)
    far = shift(ym, "y", 1)
    zp = shift(zb, "y", -1)
    zm = far_z(ym)
    zfar = far_z(far)
    return [b, ym, yp, far, zb, zp, zm, zfar]


def gather_green_y(g):
    gz = shift(g, "zh", 1)
    pair = jnp.stack([g, gz])
    ym, yp = shift(pair, "y", 1), shift(pair, "y", -1)
    far0 = shift(ym[0], "y", 1)
    far1 = shift(yp[1], "y", -1)
    far = jnp.stack([far0, far1])
    return jnp.stack([pair, ym, yp, far])


def gather_green_x(g8, x_after):
    gx = after(g8, *x_after)
    xm, xp = shift(gx, "x", 1), shift(gx, "x", -1)
    far0 = shift(xm[:2], "x", 1)
    far1 = shift(xp[2:], "x", -1)
    mine = [g8, xm, xp, far0, far1]
    every, odd = (0, 3, 1, 2), None
    plan = [(0, every), (3, every), (1, every), (2, every[:2]), (2, every[2:])]
    greens = mine + [shift(v, "core", 1) for v in mine]
    return greens, [(dx, o, dys) for o in (False, True) for dx, dys in plan]


def reduce_out(own, other, s_block, time_weights):
    zh, y, x, _ = (lax.axis_index(a) for a in GRID)
    tm = lax.axis_index("tm")
    part = own.astype(F32) + shift(other, "core", 1).astype(F32)
    part = part.reshape(2, 4, 4, 16, part.shape[-1])

    def for_x(k):
        return lax.dynamic_index_in_dim(part, lax.rem(x + k, 4), 2, keepdims=False)

    far = for_x(2).astype(BF)
    relay_up = shift(far[0], "x", 1).astype(F32)
    relay_down = shift(far[1], "x", -1).astype(F32)
    nxt, prv = for_x(1), for_x(3)
    up = jnp.stack([nxt[0] + relay_up, nxt[1]]).astype(BF)
    down = jnp.stack([prv[0], prv[1] + relay_down]).astype(BF)
    back = for_x(0) + shift(up, "x", 1).astype(F32) + shift(down, "x", -1).astype(F32)
    back = back.astype(BF).reshape(128, -1)
    coef = jnp.dot(back, s_block, preferred_element_type=F32).reshape(2, 4, 16, NB)

    def for_y(k):
        return lax.dynamic_index_in_dim(coef, lax.rem(y + k, 4), 1, keepdims=False)

    col = for_y(0)
    for k in (1, 2, 3):
        col = col + shift(for_y(k), "y", k)

    def weighted(f, z):
        w = lax.dynamic_slice(time_weights, (f, tm), (1, 1)) * (1.0 / NR)
        return w * lax.dynamic_index_in_dim(col, z, 0, keepdims=False)

    out = weighted(tm, zh)
    out = out + shift(weighted(1 - tm, zh), "tm", 1)
    out = out + shift(weighted(tm, 1 - zh), "zh", 1)
    out = out + far_z(weighted(1 - tm, 1 - zh))
    return out[None]


def shards(occupied_green, empty_green, basis, time_weights):
    g = jnp.concatenate([occupied_green, empty_green])
    s_pieces, s_far = gather_points_x(basis)
    g8 = gather_green_y(g)
    r_pieces = gather_points_yz(basis, (g8,))
    greens, plan = gather_green_x(g8, s_far)
    proj, s_block = project(s_pieces, greens, plan)
    own, other = main(proj, r_pieces)
    return reduce_out(own, other, s_block, time_weights)


def solution(mesh):
    split = Mesh(
        mesh.devices.reshape(mesh.shape["tm"], 2, 4, 4, 2),
        ("tm", "zh", "y", "x", "core"),
    )
    in_specs = (P("tm", GRID, None), P("tm", GRID, None), P(GRID, None), P())
    out_specs = P("tm", GRID, None)
    return jax.shard_map(
        shards, mesh=split, in_specs=in_specs, out_specs=out_specs, check_vma=False
    )
```

```python
import jax
import jax.numpy as jnp
from jax import lax
from jax.experimental import pallas as pl
from jax.experimental.pallas import tpu as pltpu
from jax.sharding import Mesh
from jax.sharding import PartitionSpec as P

NR = 12288
NB = 1024
GRID = ("zh", "y", "x", "core")
BF = jnp.bfloat16
F32 = jnp.float32
ANY = pl.BlockSpec(memory_space=pl.ANY)
MIB = 1024 * 1024


def shift(v, axis, step):
    n = lax.axis_size(axis)
    return lax.ppermute(v, axis, [(i, (i + step) % n) for i in range(n)])


def far_z(v):
    return lax.ppermute(v, ("tm", "zh"), [(0, 3), (3, 0), (1, 2), (2, 1)])


def after(v, *deps):
    return lax.optimization_barrier((v, *deps))[0]


def nt(a, b):
    return lax.dot_general(a, b, (((1,), (1,)), ((), ())), preferred_element_type=F32)


def copy_all(copies):
    for c in copies:
        c.start()
    for c in copies:
        c.wait()


def row_copies(pieces, dst, sems, first):
    out, row = [], 0
    for j, p in enumerate(pieces):
        rows = p.shape[0]
        out.append(pltpu.make_async_copy(p, dst.at[pl.ds(row, rows)], sems.at[first + j]))
        row += rows
    return out


RING = (0, 3, 1, 2)
DEV_ROWS = 192
R_TILE = 512
K_TILE = 256


def assemble_kernel(*refs):
    pieces, out, sems = refs[:-2], refs[-2], refs[-1]
    x, core = lax.axis_index("x"), lax.axis_index("core")
    copies = []
    for n, p in enumerate(pieces):
        cc = core if n < len(RING) else 1 - core
        row = pl.multiple_of((lax.rem(x + RING[n % 4], 4) * 2 + cc) * DEV_ROWS, 64)
        copies.append(pltpu.make_async_copy(p, out.at[pl.ds(row, DEV_ROWS)], sems.at[n]))
    copy_all(copies)


def assemble(pieces):
    rows = len(pieces) * DEV_ROWS
    return pl.pallas_call(
        assemble_kernel,
        out_shape=jax.ShapeDtypeStruct((rows, NB), BF),
        in_specs=[ANY] * len(pieces),
        out_specs=pl.BlockSpec(memory_space=pltpu.VMEM),
        scratch_shapes=[pltpu.SemaphoreType.DMA((len(pieces),))],
        compiler_params=pltpu.CompilerParams(vmem_limit_bytes=6 * MIB),
        cost_estimate=pl.CostEstimate(flops=10**9, bytes_accessed=6 * MIB, transcendentals=0),
        name="assemble",
    )(*pieces)


def main_kernel(n_r, first, s_tile, *refs):
    chunks = refs[: 2 * len(RING)]
    pieces = refs[2 * len(RING) : 2 * len(RING) + n_r]
    own_ref, other_ref, proj, block, block_t, product, r_sems, p_sems = refs[2 * len(RING) + n_r :]
    x, core = lax.axis_index("x"), lax.axis_index("core")
    r_rows = block.shape[0]
    s_rows = proj.shape[-1]

    @pl.when(pl.program_id(0) == 0)
    def _():
        r_copies = row_copies(pieces, block, r_sems, 0)
        p_copies = []
        for n, ref in enumerate(chunks):
            cc = core if n < len(RING) else 1 - core
            xx = lax.rem(x + RING[n % 4], 4)
            for zy in range(8):
                row = pl.multiple_of(((zy * 4 + xx) * 2 + cc) * 16, 16)
                for q in range(2):
                    p_copies.append(
                        pltpu.make_async_copy(
                            ref.at[zy, q, :, pl.ds(first, s_rows)],
                            proj.at[q, pl.ds(row, 16)],
                            p_sems.at[(n * 8 + zy) * 2 + q],
                        )
                    )
        for c in r_copies + p_copies:
            c.start()
        for c in r_copies:
            c.wait()

        def turn(i, carry):
            at = pl.ds(pl.multiple_of(i * 256, 256), 256)
            block_t[:, at] = block[at].T
            return carry

        lax.fori_loop(0, r_rows // 256, turn, 0)
        for c in p_copies:
            c.wait()

    cols = pl.ds(pl.multiple_of(pl.program_id(0) * s_tile, s_tile), s_tile)

    def real_space(i, carry):
        at = pl.ds(pl.multiple_of(i * R_TILE, R_TILE), R_TILE)
        rows = block[at]
        occupied = jnp.dot(rows, proj[0, :, cols], preferred_element_type=F32)
        empty = jnp.dot(rows, proj[1, :, cols], preferred_element_type=F32)
        product[at] = (occupied * empty).astype(BF)
        return carry

    lax.fori_loop(0, r_rows // R_TILE, real_space, 0)

    def back_half(i, carry):
        at = pl.ds(pl.multiple_of(i * K_TILE, K_TILE), K_TILE)
        back = jnp.dot(block_t[at], product[...], preferred_element_type=F32).astype(BF)
        groups = K_TILE // 32
        back = back.reshape(groups, 2, 16, back.shape[1])
        to = pl.ds(pl.multiple_of(i * groups, groups), groups)
        own_ref[to] = jnp.where(core == 0, back[:, 0], back[:, 1])
        other_ref[to] = jnp.where(core == 0, back[:, 1], back[:, 0])
        return carry

    lax.fori_loop(0, NB // K_TILE, back_half, 0)


def main(chunks, pieces, first, s_rows, s_tile):
    r_rows = sum(p.shape[0] for p in pieces)
    half = jax.ShapeDtypeStruct((NB // 32, 16, s_rows), BF)
    half_spec = pl.BlockSpec((NB // 32, 16, s_tile), lambda i: (0, 0, i))

    def kernel(*refs):
        main_kernel(len(pieces), first, s_tile, *refs)

    return pl.pallas_call(
        kernel,
        grid=(s_rows // s_tile,),
        out_shape=(half, half),
        in_specs=[ANY] * (len(chunks) + len(pieces)),
        out_specs=(half_spec, half_spec),
        scratch_shapes=[
            pltpu.VMEM((2, NB, s_rows), BF),
            pltpu.VMEM((r_rows, NB), BF),
            pltpu.VMEM((NB, r_rows), BF),
            pltpu.VMEM((r_rows, s_tile), BF),
            pltpu.SemaphoreType.DMA((len(pieces),)),
            pltpu.SemaphoreType.DMA((16 * len(chunks),)),
        ],
        compiler_params=pltpu.CompilerParams(vmem_limit_bytes=30 * MIB),
        cost_estimate=pl.CostEstimate(
            flops=6 * s_rows * r_rows * NB, bytes_accessed=12 * MIB, transcendentals=0
        ),
        name="main",
    )(*chunks, *pieces)


def gather_x(v):
    return [v, shift(v, "x", 1), shift(v, "x", -1), shift(v, "x", 2)]


def both_cores(parts):
    return parts + [shift(v, "core", 1) for v in parts]


def gather_points_yz(b, green):
    zb = far_z(b)
    by = after(b, green)
    ym, yp, far = shift(by, "y", 1), shift(by, "y", -1), shift(by, "y", 2)
    zp = shift(after(zb, green), "y", -1)
    zm = far_z(ym)
    zfar = far_z(far)
    return [b, ym, yp, far, zb, zp, zm, zfar]


def project(green, s_block):
    rows = nt(green.reshape(-1, NB), s_block).astype(BF)
    return rows.reshape(*green.shape[:-1], s_block.shape[0])


def sum_over_x(own, other):
    x = lax.axis_index("x")
    part = own.astype(F32) + shift(other, "core", 1).astype(F32)
    part = part.reshape(8, 4, 16, part.shape[-1])

    def for_x(k):
        return lax.dynamic_index_in_dim(part, lax.rem(x + k, 4), 1, keepdims=False)

    sent = [shift(for_x(k).astype(BF), "x", k) for k in (1, 3, 2)]
    return for_x(0), sent


def finish(mine, sent):
    back = mine
    for v in sent:
        back = back + v.astype(F32)
    return back.astype(BF).reshape(128, -1)


def reduce_out(coef, time_weights):
    zh, y = lax.axis_index("zh"), lax.axis_index("y")
    tm = lax.axis_index("tm")
    coef = coef.reshape(2, 4, 16, NB)

    def for_y(k):
        return lax.dynamic_index_in_dim(coef, lax.rem(y + k, 4), 1, keepdims=False)

    col = for_y(0)
    for k in (1, 3, 2):
        col = col + shift(for_y(k), "y", k)

    def weighted(f, z):
        w = lax.dynamic_slice(time_weights, (f, tm), (1, 1)) * (1.0 / NR)
        return w * lax.dynamic_index_in_dim(col, z, 0, keepdims=False)

    out = weighted(tm, zh)
    out = out + shift(weighted(1 - tm, zh), "tm", 1)
    out = out + shift(weighted(tm, 1 - zh), "zh", 1)
    out = out + far_z(weighted(1 - tm, 1 - zh))
    return out[None]


def shards(occupied_green, empty_green, basis, time_weights):
    green = jnp.concatenate([occupied_green, empty_green])
    s_pieces = both_cores(gather_x(basis))
    green = lax.all_gather(green, ("zh", "y"), axis=0, tiled=False)
    r_pieces = gather_points_yz(basis, green)
    greens = gather_x(green)
    s_block = assemble(s_pieces)
    chunks = both_cores([project(v, s_block) for v in greens])
    rows = s_block.shape[0]
    own, other = main(chunks, r_pieces, 0, s_block.shape[0], 512)
    mine, sent = sum_over_x(own, other)
    coef = jnp.dot(finish(mine, sent), s_block, preferred_element_type=F32)
    return reduce_out(coef, time_weights)


def solution(mesh):
    split = Mesh(
        mesh.devices.reshape(mesh.shape["tm"], 2, 4, 4, 2),
        ("tm", "zh", "y", "x", "core"),
    )
    in_specs = (P("tm", GRID, None), P("tm", GRID, None), P(GRID, None), P())
    out_specs = P("tm", GRID, None)
    return jax.shard_map(
        shards, mesh=split, in_specs=in_specs, out_specs=out_specs, check_vma=False
    )
```

```python
import jax
import jax.numpy as jnp
from jax import lax
from jax.experimental import pallas as pl
from jax.experimental.pallas import tpu as pltpu
from jax.sharding import Mesh
from jax.sharding import PartitionSpec as P

NR = 12288
NB = 1024
GRID = ("zh", "y", "x", "core")
BF = jnp.bfloat16
F32 = jnp.float32
ANY = pl.BlockSpec(memory_space=pl.ANY)
MIB = 1024 * 1024


def shift(v, axis, step):
    n = lax.axis_size(axis)
    return lax.ppermute(v, axis, [(i, (i + step) % n) for i in range(n)])


def far_z(v):
    return lax.ppermute(v, ("tm", "zh"), [(0, 3), (3, 0), (1, 2), (2, 1)])


def after(v, *deps):
    return lax.optimization_barrier((v, *deps))[0]


def nt(a, b):
    return lax.dot_general(a, b, (((1,), (1,)), ((), ())), preferred_element_type=F32)


def copy_all(copies):
    for c in copies:
        c.start()
    for c in copies:
        c.wait()


def row_copies(pieces, dst, sems, first):
    out, row = [], 0
    for j, p in enumerate(pieces):
        rows = p.shape[0]
        out.append(pltpu.make_async_copy(p, dst.at[pl.ds(row, rows)], sems.at[first + j]))
        row += rows
    return out


RING = (0, 3, 1, 2)
DEV_ROWS = 192
R_TILE = 512


def assemble_kernel(*refs):
    pieces, out, sems = refs[:-2], refs[-2], refs[-1]
    x, tm = lax.axis_index("x"), lax.axis_index("tm")
    half = DEV_ROWS // 2
    copies = []
    for n, p in enumerate(pieces):
        row = lax.rem(x + S_RING[n], 4) * DEV_ROWS
        if n >= 3:
            row += half * (tm if n == 3 else 1 - tm)
        to = out.at[pl.ds(pl.multiple_of(row, 32), p.shape[0])]
        copies.append(pltpu.make_async_copy(p, to, sems.at[n]))
    copy_all(copies)


def assemble(pieces):
    return pl.pallas_call(
        assemble_kernel,
        out_shape=jax.ShapeDtypeStruct((4 * DEV_ROWS, NB), BF),
        in_specs=[ANY] * len(pieces),
        out_specs=pl.BlockSpec(memory_space=pltpu.VMEM),
        scratch_shapes=[pltpu.SemaphoreType.DMA((len(pieces),))],
        compiler_params=pltpu.CompilerParams(vmem_limit_bytes=6 * MIB),
        cost_estimate=pl.CostEstimate(flops=10**9, bytes_accessed=6 * MIB, transcendentals=0),
        name="assemble",
    )(*pieces)


def main_kernel(n_r, *refs):
    n_c = 2 * len(RING)
    chunks = refs[:n_c]
    pieces = refs[n_c : n_c + n_r]
    outs = refs[n_c + n_r : n_c + n_r + 4]
    proj, block, block_t, product, r_sems, p_sems = refs[n_c + n_r + 4 :]
    x, core = lax.axis_index("x"), lax.axis_index("core")
    r_rows = block.shape[0]
    s_rows = proj.shape[-1]
    r_copies = row_copies(pieces, block, r_sems, 0)
    p_copies = []
    for n, ref in enumerate(chunks):
        cc = core if n < len(RING) else 1 - core
        xc = lax.rem(x + RING[n % 4], 4) * 2 + cc
        for q in range(2):
            p_copies.append(
                pltpu.make_async_copy(ref.at[q], proj.at[q, :, xc], p_sems.at[2 * n + q])
            )
    for c in r_copies + p_copies:
        c.start()
    for c in r_copies:
        c.wait()

    def turn(i, carry):
        at = pl.ds(pl.multiple_of(i * 256, 256), 256)
        block_t[:, :, :, at] = block[at].T.reshape(8, 4, 32, 256)
        return carry

    lax.fori_loop(0, r_rows // 256, turn, 0)
    for c in p_copies:
        c.wait()

    def real_space(i, carry):
        at = pl.ds(pl.multiple_of(i * R_TILE, R_TILE), R_TILE)
        rows = block[at]
        occupied = jnp.dot(rows, proj[0].reshape(NB, s_rows), preferred_element_type=F32)
        empty = jnp.dot(rows, proj[1].reshape(NB, s_rows), preferred_element_type=F32)
        product[at] = (occupied * empty).astype(BF)
        return carry

    lax.fori_loop(0, r_rows // R_TILE, real_space, 0)
    for k in range(4):
        rows = block_t[:, lax.rem(x + k, 4)].reshape(NB // 4, r_rows)
        back = jnp.dot(rows, product[...], preferred_element_type=F32).astype(BF)
        outs[k][...] = back.reshape(8, 32, s_rows)


def main(chunks, pieces, s_rows):
    r_rows = sum(p.shape[0] for p in pieces)

    def kernel(*refs):
        main_kernel(len(pieces), *refs)

    return pl.pallas_call(
        kernel,
        out_shape=[jax.ShapeDtypeStruct((8, 32, s_rows), BF)] * 4,
        in_specs=[ANY] * (len(chunks) + len(pieces)),
        out_specs=[pl.BlockSpec(memory_space=pltpu.VMEM)] * 4,
        scratch_shapes=[
            pltpu.VMEM((2, 8, 8, 16, s_rows), BF),
            pltpu.VMEM((r_rows, NB), BF),
            pltpu.VMEM((8, 4, 32, r_rows), BF),
            pltpu.VMEM((r_rows, s_rows), BF),
            pltpu.SemaphoreType.DMA((len(pieces),)),
            pltpu.SemaphoreType.DMA((2 * len(chunks),)),
        ],
        compiler_params=pltpu.CompilerParams(vmem_limit_bytes=32 * MIB),
        cost_estimate=pl.CostEstimate(
            flops=6 * s_rows * r_rows * NB, bytes_accessed=12 * MIB, transcendentals=0
        ),
        name="main",
    )(*chunks, *pieces)


def gather_x(v):
    return [v, shift(v, "x", 1), shift(v, "x", -1), shift(v, "x", 2)]


def both_cores(parts):
    return parts + [shift(v, "core", 1) for v in parts]


S_RING = (0, 3, 1, 2, 2)


def gather_points_x(b):
    half = DEV_ROWS // 2
    part = lax.dynamic_slice_in_dim(b, lax.axis_index("tm") * half, half, 0)
    xm, xp, far = shift(b, "x", 1), shift(b, "x", -1), shift(part, "x", 2)
    return [b, xm, xp, far, shift(far, "tm", 1)]


def gather_points_yz(b, green):
    zb = far_z(b)
    by = after(b, green)
    ym, yp, far = shift(by, "y", 1), shift(by, "y", -1), shift(by, "y", 2)
    zp = shift(after(zb, green), "y", -1)
    zm = far_z(ym)
    zfar = far_z(far)
    return [b, ym, yp, far, zb, zp, zm, zfar]


def gather_green_yz(g):
    zh, y = lax.axis_index("zh"), lax.axis_index("y")
    gz = shift(g, "zh", 1)
    first = zh == 0
    pair = jnp.stack([jnp.where(first, g, gz), jnp.where(first, gz, g)], axis=1)
    parts = [pair, shift(pair, "y", -1), shift(pair, "y", 2), shift(pair, "y", 1)]
    out = jnp.zeros((2, 2, 4, 16, NB), BF)
    for k, v in enumerate(parts):
        out = lax.dynamic_update_slice_in_dim(out, v[:, :, None], lax.rem(y + k, 4), 2)
    return out.reshape(2, 8, 16, NB)


def project(green, s_block):
    rows = nt(green.reshape(-1, NB), s_block).astype(BF)
    return rows.reshape(*green.shape[:-1], s_block.shape[0])


def sum_over_x(parts):
    back = parts[0].astype(F32)
    for k in (2, 1, 3):
        back = back + shift(parts[k], "x", k).astype(F32)
    return back.astype(BF).reshape(256, -1)


def reduce_out(coef, time_weights):
    zh, y, core = (lax.axis_index(a) for a in ("zh", "y", "core"))
    tm = lax.axis_index("tm")
    coef = coef.reshape(8, 2, 16, NB)

    def for_core(k):
        return lax.dynamic_index_in_dim(coef, k, 1, keepdims=False)

    coef = for_core(core) + shift(for_core(1 - core), "core", 1)
    coef = coef.reshape(2, 4, 16, NB)

    def for_y(k):
        return lax.dynamic_index_in_dim(coef, lax.rem(y + k, 4), 1, keepdims=False)

    col = for_y(0)
    for k in (1, 3, 2):
        col = col + shift(for_y(k), "y", k)

    def weighted(f, z):
        w = lax.dynamic_slice(time_weights, (f, tm), (1, 1)) * (1.0 / NR)
        return w * lax.dynamic_index_in_dim(col, z, 0, keepdims=False)

    out = weighted(tm, zh)
    out = out + shift(weighted(1 - tm, zh), "tm", 1)
    out = out + shift(weighted(tm, 1 - zh), "zh", 1)
    out = out + far_z(weighted(1 - tm, 1 - zh))
    return out[None]


def shards(occupied_green, empty_green, basis, time_weights):
    green = jnp.concatenate([occupied_green, empty_green])
    green = gather_green_yz(green)
    s_block = assemble(gather_points_x(basis))
    r_pieces = both_cores(gather_points_yz(basis, green))
    greens = both_cores(gather_x(green))
    chunks = [project(v, s_block) for v in greens]
    parts = main(chunks, r_pieces, s_block.shape[0])
    coef = jnp.dot(sum_over_x(parts), s_block, preferred_element_type=F32)
    return reduce_out(coef, time_weights)


def solution(mesh):
    split = Mesh(
        mesh.devices.reshape(mesh.shape["tm"], 2, 4, 4, 2),
        ("tm", "zh", "y", "x", "core"),
    )
    in_specs = (P("tm", GRID, None), P("tm", GRID, None), P(GRID, None), P())
    out_specs = P("tm", GRID, None)
    return jax.shard_map(
        shards, mesh=split, in_specs=in_specs, out_specs=out_specs, check_vma=False
    )
```

```python
import jax
import jax.numpy as jnp
from jax import lax
from jax.experimental import pallas as pl
from jax.experimental.pallas import tpu as pltpu
from jax.sharding import Mesh
from jax.sharding import PartitionSpec as P


NR = 12288
NB = 1024
GRID = ("zh", "y", "x", "core")
BF = jnp.bfloat16
F32 = jnp.float32
ANY = pl.BlockSpec(memory_space=pl.ANY)
MIB = 1024 * 1024


def shift(v, axis, step):
    n = lax.axis_size(axis)
    return lax.ppermute(v, axis, [(i, (i + step) % n) for i in range(n)])


def far_z(v):
    return lax.ppermute(v, ("tm", "zh"), [(0, 3), (3, 0), (1, 2), (2, 1)])


def nt(a, b):
    return lax.dot_general(a, b, (((1,), (1,)), ((), ())), preferred_element_type=F32)


def copy_all(copies):
    for c in copies:
        c.start()
    for c in copies:
        c.wait()


def row_copies(pieces, dst, sems, first):
    out, row = [], 0
    for j, p in enumerate(pieces):
        rows = p.shape[0]
        out.append(pltpu.make_async_copy(p, dst.at[pl.ds(row, rows)], sems.at[first + j]))
        row += rows
    return out


RING = (0, 3, 1, 2)
DEV_ROWS = 192
R_TILE = 512


def assemble_kernel(*refs):
    pieces, out, sems = refs[:-2], refs[-2], refs[-1]
    x, tm = lax.axis_index("x"), lax.axis_index("tm")
    half = DEV_ROWS // 2
    copies = []
    for n, p in enumerate(pieces):
        row = lax.rem(x + S_RING[n], 4) * DEV_ROWS
        if n >= 3:
            row += half * (tm if n == 3 else 1 - tm)
        to = out.at[pl.ds(pl.multiple_of(row, 32), p.shape[0])]
        copies.append(pltpu.make_async_copy(p, to, sems.at[n]))
    copy_all(copies)


def assemble(pieces):
    return pl.pallas_call(
        assemble_kernel,
        out_shape=jax.ShapeDtypeStruct((4 * DEV_ROWS, NB), BF),
        in_specs=[ANY] * len(pieces),
        out_specs=pl.BlockSpec(memory_space=pltpu.VMEM),
        scratch_shapes=[pltpu.SemaphoreType.DMA((len(pieces),))],
        compiler_params=pltpu.CompilerParams(vmem_limit_bytes=6 * MIB),
        cost_estimate=pl.CostEstimate(flops=10**9, bytes_accessed=6 * MIB, transcendentals=0),
        name="assemble",
    )(*pieces)


def main_kernel(n_r, *refs):
    n_c = 2 * len(RING)
    chunks = refs[:n_c]
    pieces = refs[n_c : n_c + n_r]
    outs = refs[n_c + n_r : n_c + n_r + 4]
    proj, block, block_t, product, r_sems, p_sems = refs[n_c + n_r + 4 :]
    x, core = lax.axis_index("x"), lax.axis_index("core")
    r_rows = block.shape[0]
    s_rows = proj.shape[-1]
    r_copies = row_copies(pieces, block, r_sems, 0)
    p_copies = []
    for n, ref in enumerate(chunks):
        cc = core if n < len(RING) else 1 - core
        xc = lax.rem(x + RING[n % 4], 4) * 2 + cc
        for q in range(2):
            p_copies.append(
                pltpu.make_async_copy(ref.at[q], proj.at[q, :, xc], p_sems.at[2 * n + q])
            )
    for c in p_copies + r_copies:
        c.start()
    for c in p_copies:
        c.wait()

    def real_space(i, carry):
        at = pl.ds(pl.multiple_of(i * R_TILE, R_TILE), R_TILE)
        rows = block[at]
        occupied = jnp.dot(rows, proj[0].reshape(NB, s_rows), preferred_element_type=F32)
        empty = jnp.dot(rows, proj[1].reshape(NB, s_rows), preferred_element_type=F32)
        product[at] = (occupied * empty).astype(BF)
        block_t[:, :, :, at] = rows.T.reshape(8, 4, 32, R_TILE)
        return carry

    tiles = r_rows // R_TILE
    for part in range(2):
        for c in r_copies[part * n_r // 2 : (part + 1) * n_r // 2]:
            c.wait()
        lax.fori_loop(part * tiles // 2, (part + 1) * tiles // 2, real_space, 0)
    for k in range(4):
        rows = block_t[:, lax.rem(x + k, 4)].reshape(NB // 4, r_rows)
        back = jnp.dot(rows, product[...], preferred_element_type=F32).astype(BF)
        outs[k][...] = back.reshape(8, 32, s_rows)


def main(chunks, pieces, s_rows):
    r_rows = sum(p.shape[0] for p in pieces)

    def kernel(*refs):
        main_kernel(len(pieces), *refs)

    return pl.pallas_call(
        kernel,
        out_shape=[jax.ShapeDtypeStruct((8, 32, s_rows), BF)] * 4,
        in_specs=[ANY] * (len(chunks) + len(pieces)),
        out_specs=[pl.BlockSpec(memory_space=pltpu.VMEM)] * 4,
        scratch_shapes=[
            pltpu.VMEM((2, 8, 8, 16, s_rows), BF),
            pltpu.VMEM((r_rows, NB), BF),
            pltpu.VMEM((8, 4, 32, r_rows), BF),
            pltpu.VMEM((r_rows, s_rows), BF),
            pltpu.SemaphoreType.DMA((len(pieces),)),
            pltpu.SemaphoreType.DMA((2 * len(chunks),)),
        ],
        compiler_params=pltpu.CompilerParams(vmem_limit_bytes=32 * MIB),
        cost_estimate=pl.CostEstimate(
            flops=6 * s_rows * r_rows * NB, bytes_accessed=12 * MIB, transcendentals=0
        ),
        name="main",
    )(*chunks, *pieces)


def gather_x(v):
    return [v, shift(v, "x", 1), shift(v, "x", -1), shift(v, "x", 2)]


def both_cores(parts):
    return parts + [shift(v, "core", 1) for v in parts]


S_RING = (0, 3, 1, 2, 2)


def gather_points_x(b):
    half = DEV_ROWS // 2
    part = lax.dynamic_slice_in_dim(b, lax.axis_index("tm") * half, half, 0)
    xm, xp, far = shift(b, "x", 1), shift(b, "x", -1), shift(part, "x", 2)
    return [b, xm, xp, far, shift(far, "tm", 1)]


def gather_points_yz(b):
    zb = far_z(b)
    ym, yp, far = shift(b, "y", 1), shift(b, "y", -1), shift(b, "y", 2)
    zm = far_z(ym)
    zfar = far_z(far)
    zp = shift(zb, "y", -1)
    return [b, ym, yp, far, zb, zp, zm, zfar]


def gather_green_yz(g):
    zh, y = lax.axis_index("zh"), lax.axis_index("y")
    gz = shift(g, "zh", 1)
    first = zh == 0
    pair = jnp.stack([jnp.where(first, g, gz), jnp.where(first, gz, g)], axis=1)
    parts = [pair, shift(pair, "y", -1), shift(pair, "y", 2), shift(pair, "y", 1)]
    out = jnp.zeros((2, 2, 4, 16, NB), BF)
    for k, v in enumerate(parts):
        out = lax.dynamic_update_slice_in_dim(out, v[:, :, None], lax.rem(y + k, 4), 2)
    return out.reshape(2, 8, 16, NB)


def project(green, s_block):
    rows = nt(green.reshape(-1, NB), s_block).astype(BF)
    return rows.reshape(*green.shape[:-1], s_block.shape[0])


def sum_over_x(parts):
    back = parts[0].astype(F32)
    for k in (2, 1, 3):
        back = back + shift(parts[k], "x", k).astype(F32)
    return back.astype(BF).reshape(256, -1)


def reduce_out(coef, time_weights):
    zh, y, core = (lax.axis_index(a) for a in ("zh", "y", "core"))
    tm = lax.axis_index("tm")
    coef = coef.reshape(8, 2, 16, NB)

    def for_core(k):
        return lax.dynamic_index_in_dim(coef, k, 1, keepdims=False)

    coef = for_core(core) + shift(for_core(1 - core), "core", 1)
    coef = coef.reshape(2, 4, 16, NB)

    def for_y(k):
        return lax.dynamic_index_in_dim(coef, lax.rem(y + k, 4), 1, keepdims=False)

    col = for_y(0)
    for k in (1, 3, 2):
        col = col + shift(for_y(k), "y", k)

    def weighted(f, z):
        w = lax.dynamic_slice(time_weights, (f, tm), (1, 1)) * (1.0 / NR)
        return w * lax.dynamic_index_in_dim(col, z, 0, keepdims=False)

    out = weighted(tm, zh)
    out = out + shift(weighted(1 - tm, zh), "tm", 1)
    out = out + shift(weighted(tm, 1 - zh), "zh", 1)
    out = out + far_z(weighted(1 - tm, 1 - zh))
    return out[None]


def shards(occupied_green, empty_green, basis, time_weights):
    green = jnp.stack([occupied_green[0], empty_green[0]])
    green = gather_green_yz(green)
    s_pieces = gather_points_x(basis)
    s_block = assemble(s_pieces)
    r_pieces = both_cores(gather_points_yz(basis))
    greens = both_cores(gather_x(green))
    chunks = [project(v, s_block) for v in greens]
    parts = main(chunks, r_pieces, s_block.shape[0])
    coef = jnp.dot(sum_over_x(parts), s_block, preferred_element_type=F32)
    return reduce_out(coef, time_weights)


def solution(mesh):
    split = Mesh(
        mesh.devices.reshape(mesh.shape["tm"], 2, 4, 4, 2),
        ("tm", "zh", "y", "x", "core"),
    )
    in_specs = (P("tm", GRID, None), P("tm", GRID, None), P(GRID, None), P())
    out_specs = P("tm", GRID, None)

    return jax.shard_map(
        shards, mesh=split, in_specs=in_specs, out_specs=out_specs, check_vma=False
    )
```

```python
import jax
import jax.numpy as jnp
from jax import lax
from jax.experimental import pallas as pl
from jax.experimental.pallas import tpu as pltpu
from jax.sharding import Mesh
from jax.sharding import PartitionSpec as P


NR = 12288
NB = 1024
GRID = ("zh", "y", "x", "core")
BF = jnp.bfloat16
F32 = jnp.float32
ANY = pl.BlockSpec(memory_space=pl.ANY)
MIB = 1024 * 1024


def shift(v, axis, step):
    n = lax.axis_size(axis)
    return lax.ppermute(v, axis, [(i, (i + step) % n) for i in range(n)])


def far_z(v):
    return lax.ppermute(v, ("tm", "zh"), [(0, 3), (3, 0), (1, 2), (2, 1)])


def nt(a, b):
    return lax.dot_general(a, b, (((1,), (1,)), ((), ())), preferred_element_type=F32)


def copy_all(copies):
    for c in copies:
        c.start()
    for c in copies:
        c.wait()


def row_copies(pieces, dst, sems, first):
    out, row = [], 0
    for j, p in enumerate(pieces):
        rows = p.shape[0]
        out.append(pltpu.make_async_copy(p, dst.at[pl.ds(row, rows)], sems.at[first + j]))
        row += rows
    return out


RING = (0, 3, 1, 2)
DEV_ROWS = 192
R_TILE = 512


def assemble_kernel(*refs):
    pieces, out, sems = refs[:-2], refs[-2], refs[-1]
    x, tm = lax.axis_index("x"), lax.axis_index("tm")
    half = DEV_ROWS // 2
    copies = []
    for n, p in enumerate(pieces):
        row = lax.rem(x + S_RING[n], 4) * DEV_ROWS
        if n >= 3:
            row += half * (tm if n == 3 else 1 - tm)
        to = out.at[pl.ds(pl.multiple_of(row, 32), p.shape[0])]
        copies.append(pltpu.make_async_copy(p, to, sems.at[n]))
    copy_all(copies)


def assemble(pieces):
    return pl.pallas_call(
        assemble_kernel,
        out_shape=jax.ShapeDtypeStruct((4 * DEV_ROWS, NB), BF),
        in_specs=[ANY] * len(pieces),
        out_specs=pl.BlockSpec(memory_space=pltpu.VMEM),
        scratch_shapes=[pltpu.SemaphoreType.DMA((len(pieces),))],
        compiler_params=pltpu.CompilerParams(vmem_limit_bytes=6 * MIB),
        cost_estimate=pl.CostEstimate(flops=10**9, bytes_accessed=6 * MIB, transcendentals=0),
        name="assemble",
    )(*pieces)


def main_kernel(n_r, *refs):
    n_c = 2 * len(RING)
    chunks = refs[:n_c]
    pieces = refs[n_c : n_c + n_r]
    outs = refs[n_c + n_r : n_c + n_r + 4]
    proj, block, block_t, product, r_sems, p_sems = refs[n_c + n_r + 4 :]
    x, core = lax.axis_index("x"), lax.axis_index("core")
    r_rows = block.shape[0]
    s_rows = proj.shape[-1]
    r_copies = row_copies(pieces, block, r_sems, 0)
    p_copies = []
    for n, ref in enumerate(chunks):
        cc = core if n < len(RING) else 1 - core
        xc = lax.rem(x + RING[n % 4], 4) * 2 + cc
        for q in range(2):
            p_copies.append(
                pltpu.make_async_copy(ref.at[q], proj.at[q, :, xc], p_sems.at[2 * n + q])
            )
    for c in p_copies + r_copies:
        c.start()
    for c in p_copies:
        c.wait()

    def real_space(i, carry):
        at = pl.ds(pl.multiple_of(i * R_TILE, R_TILE), R_TILE)
        rows = block[at]
        occupied = jnp.dot(rows, proj[0].reshape(NB, s_rows), preferred_element_type=F32)
        empty = jnp.dot(rows, proj[1].reshape(NB, s_rows), preferred_element_type=F32)
        product[at] = (occupied * empty).astype(BF)
        block_t[:, :, :, at] = rows.T.reshape(8, 4, 32, R_TILE)
        return carry

    tiles = r_rows // R_TILE
    for part in range(2):
        for c in r_copies[part * n_r // 2 : (part + 1) * n_r // 2]:
            c.wait()
        lax.fori_loop(part * tiles // 2, (part + 1) * tiles // 2, real_space, 0)
    for k in range(4):
        rows = block_t[:, lax.rem(x + k, 4)].reshape(NB // 4, r_rows)
        back = jnp.dot(rows, product[...], preferred_element_type=F32).astype(BF)
        outs[k][...] = back.reshape(8, 32, s_rows)


def main(chunks, pieces, s_rows):
    r_rows = sum(p.shape[0] for p in pieces)

    def kernel(*refs):
        main_kernel(len(pieces), *refs)

    return pl.pallas_call(
        kernel,
        out_shape=[jax.ShapeDtypeStruct((8, 32, s_rows), BF)] * 4,
        in_specs=[ANY] * (len(chunks) + len(pieces)),
        out_specs=[pl.BlockSpec(memory_space=pltpu.VMEM)] * 4,
        scratch_shapes=[
            pltpu.VMEM((2, 8, 8, 16, s_rows), BF),
            pltpu.VMEM((r_rows, NB), BF),
            pltpu.VMEM((8, 4, 32, r_rows), BF),
            pltpu.VMEM((r_rows, s_rows), BF),
            pltpu.SemaphoreType.DMA((len(pieces),)),
            pltpu.SemaphoreType.DMA((2 * len(chunks),)),
        ],
        compiler_params=pltpu.CompilerParams(vmem_limit_bytes=32 * MIB),
        cost_estimate=pl.CostEstimate(
            flops=6 * s_rows * r_rows * NB, bytes_accessed=12 * MIB, transcendentals=0
        ),
        name="main",
    )(*chunks, *pieces)


def gather_green_x(v):
    xm, xp = shift(v, "x", 1), shift(v, "x", -1)
    far = jnp.stack([shift(xm[0], "x", 1), shift(xp[1], "x", -1)])
    return [v, xm, xp, far]


def both_cores(parts):
    return parts + [shift(v, "core", 1) for v in parts]


S_RING = (0, 3, 1, 2, 2)


def gather_points_x(b):
    half = DEV_ROWS // 2
    part = lax.dynamic_slice_in_dim(b, lax.axis_index("tm") * half, half, 0)
    xm, xp, far = shift(b, "x", 1), shift(b, "x", -1), shift(part, "x", 2)
    return [b, xm, xp, far, shift(far, "tm", 1)]


def gather_points_yz(b):
    far = shift(b, "y", 2)
    pair = jnp.concatenate([b, far_z(b)])
    ym, yp = shift(pair, "y", 1), shift(pair, "y", -1)
    zfar = far_z(far)
    return [pair, far, ym, zfar, yp]


def gather_green_yz(g):
    zh, y = lax.axis_index("zh"), lax.axis_index("y")
    gz = shift(g, "zh", 1)
    first = zh == 0
    pair = jnp.stack([jnp.where(first, g, gz), jnp.where(first, gz, g)], axis=1)
    parts = [pair, shift(pair, "y", -1), shift(pair, "y", 2), shift(pair, "y", 1)]
    out = jnp.zeros((2, 2, 4, 16, NB), BF)
    for k, v in enumerate(parts):
        out = lax.dynamic_update_slice_in_dim(out, v[:, :, None], lax.rem(y + k, 4), 2)
    return out.reshape(2, 8, 16, NB)


def project(green, s_block):
    rows = nt(green.reshape(-1, NB), s_block).astype(BF)
    return rows.reshape(*green.shape[:-1], s_block.shape[0])


def sum_over_x(parts):
    back = parts[0].astype(F32)
    for k in (2, 1, 3):
        back = back + shift(parts[k], "x", k).astype(F32)
    return back.astype(BF).reshape(256, -1)


def reduce_out(coef, time_weights):
    zh, y, core = (lax.axis_index(a) for a in ("zh", "y", "core"))
    tm = lax.axis_index("tm")
    coef = coef.reshape(8, 2, 16, NB)

    def for_core(k):
        return lax.dynamic_index_in_dim(coef, k, 1, keepdims=False)

    coef = for_core(core) + shift(for_core(1 - core), "core", 1)
    coef = coef.reshape(2, 4, 16, NB)

    def for_y(k):
        return lax.dynamic_index_in_dim(coef, lax.rem(y + k, 4), 1, keepdims=False)

    col = for_y(0)
    for k in (1, 3, 2):
        col = col + shift(for_y(k), "y", k)

    def weighted(f, z):
        w = lax.dynamic_slice(time_weights, (f, tm), (1, 1)) * (1.0 / NR)
        return w * lax.dynamic_index_in_dim(col, z, 0, keepdims=False)

    out = weighted(tm, zh)
    out = out + shift(weighted(1 - tm, zh), "tm", 1)
    out = out + shift(weighted(tm, 1 - zh), "zh", 1)
    out = out + far_z(weighted(1 - tm, 1 - zh))
    return out[None]


def shards(occupied_green, empty_green, basis, time_weights):
    lowest = jnp.array(-jnp.inf, BF)
    none, both = (0, 0, 0), (0, 1, 0)
    green = jnp.maximum(
        lax.pad(occupied_green, lowest, (both, none, none)),
        lax.pad(empty_green, lowest, ((1, 0, 0), none, none)),
    )
    green = gather_green_yz(green)
    s_pieces = gather_points_x(basis)
    s_block = assemble(s_pieces)
    r_pieces = both_cores(gather_points_yz(basis))
    greens = both_cores(gather_green_x(green))
    chunks = [project(v, s_block) for v in greens]
    parts = main(chunks, r_pieces, s_block.shape[0])
    coef = jnp.dot(sum_over_x(parts), s_block, preferred_element_type=F32)
    return reduce_out(coef, time_weights)


def solution(mesh):
    split = Mesh(
        mesh.devices.reshape(mesh.shape["tm"], 2, 4, 4, 2),
        ("tm", "zh", "y", "x", "core"),
    )
    in_specs = (P("tm", GRID, None), P("tm", GRID, None), P(GRID, None), P())
    out_specs = P("tm", GRID, None)

    return jax.shard_map(
        shards, mesh=split, in_specs=in_specs, out_specs=out_specs, check_vma=False
    )
```

```python
import jax
import jax.numpy as jnp
from jax import lax
from jax.experimental import pallas as pl
from jax.experimental.pallas import tpu as pltpu
from jax.sharding import Mesh
from jax.sharding import PartitionSpec as P


NR = 12288
NB = 1024
GRID = ("zh", "y", "x", "core")
BF = jnp.bfloat16
F32 = jnp.float32
ANY = pl.BlockSpec(memory_space=pl.ANY)
MIB = 1024 * 1024


def shift(v, axis, step):
    n = lax.axis_size(axis)
    return lax.ppermute(v, axis, [(i, (i + step) % n) for i in range(n)])


def far_z(v):
    return lax.ppermute(v, ("tm", "zh"), [(0, 3), (3, 0), (1, 2), (2, 1)])


def nt(a, b):
    return lax.dot_general(a, b, (((1,), (1,)), ((), ())), preferred_element_type=F32)


def copy_all(copies):
    for c in copies:
        c.start()
    for c in copies:
        c.wait()


def row_copies(pieces, dst, sems, first):
    out, row = [], 0
    for j, p in enumerate(pieces):
        rows = p.shape[0]
        out.append(pltpu.make_async_copy(p, dst.at[pl.ds(row, rows)], sems.at[first + j]))
        row += rows
    return out


RING = (0, 3, 1, 2)
DEV_ROWS = 192
R_TILE = 512


def assemble_kernel(*refs):
    pieces, out, sems = refs[:-2], refs[-2], refs[-1]
    x, tm = lax.axis_index("x"), lax.axis_index("tm")
    half = DEV_ROWS // 2
    copies = []
    for n, p in enumerate(pieces):
        row = lax.rem(x + S_RING[n], 4) * DEV_ROWS
        if n >= 3:
            row += half * (tm if n == 3 else 1 - tm)
        to = out.at[pl.ds(pl.multiple_of(row, 32), p.shape[0])]
        copies.append(pltpu.make_async_copy(p, to, sems.at[n]))
    copy_all(copies)


def assemble(pieces):
    return pl.pallas_call(
        assemble_kernel,
        out_shape=jax.ShapeDtypeStruct((4 * DEV_ROWS, NB), BF),
        in_specs=[ANY] * len(pieces),
        out_specs=pl.BlockSpec(memory_space=pltpu.VMEM),
        scratch_shapes=[pltpu.SemaphoreType.DMA((len(pieces),))],
        compiler_params=pltpu.CompilerParams(vmem_limit_bytes=6 * MIB),
        cost_estimate=pl.CostEstimate(flops=10**9, bytes_accessed=6 * MIB, transcendentals=0),
        name="assemble",
    )(*pieces)


def main_kernel(n_r, *refs):
    n_c = 2 * len(RING)
    chunks = refs[:n_c]
    pieces = refs[n_c : n_c + n_r]
    outs = refs[n_c + n_r : n_c + n_r + 4]
    proj, block, block_t, product, r_sems, p_sems = refs[n_c + n_r + 4 :]
    x, core = lax.axis_index("x"), lax.axis_index("core")
    r_rows = block.shape[0]
    s_rows = proj.shape[-1]
    r_copies = row_copies(pieces, block, r_sems, 0)
    p_copies = []
    for n, ref in enumerate(chunks):
        cc = core if n < len(RING) else 1 - core
        xc = lax.rem(x + RING[n % 4], 4) * 2 + cc
        for q in range(2):
            p_copies.append(
                pltpu.make_async_copy(ref.at[q], proj.at[q, :, xc], p_sems.at[2 * n + q])
            )
    for c in p_copies + r_copies:
        c.start()
    for c in p_copies:
        c.wait()

    def real_space(i, carry):
        at = pl.ds(pl.multiple_of(i * R_TILE, R_TILE), R_TILE)
        rows = block[at]
        occupied = jnp.dot(rows, proj[0].reshape(NB, s_rows), preferred_element_type=F32)
        empty = jnp.dot(rows, proj[1].reshape(NB, s_rows), preferred_element_type=F32)
        product[at] = (occupied * empty).astype(BF)
        block_t[:, :, :, at] = rows.T.reshape(8, 4, 32, R_TILE)
        return carry

    tiles = r_rows // R_TILE
    for part in range(2):
        for c in r_copies[part * n_r // 2 : (part + 1) * n_r // 2]:
            c.wait()
        lax.fori_loop(part * tiles // 2, (part + 1) * tiles // 2, real_space, 0)
    for k in range(4):
        rows = block_t[:, lax.rem(x + k, 4)].reshape(NB // 4, r_rows)
        back = jnp.dot(rows, product[...], preferred_element_type=F32).astype(BF)
        outs[k][...] = back.reshape(8, 32, s_rows)


def main(chunks, pieces, s_rows):
    r_rows = sum(p.shape[0] for p in pieces)

    def kernel(*refs):
        main_kernel(len(pieces), *refs)

    return pl.pallas_call(
        kernel,
        out_shape=[jax.ShapeDtypeStruct((8, 32, s_rows), BF)] * 4,
        in_specs=[ANY] * (len(chunks) + len(pieces)),
        out_specs=[pl.BlockSpec(memory_space=pltpu.VMEM)] * 4,
        scratch_shapes=[
            pltpu.VMEM((2, 8, 8, 16, s_rows), BF),
            pltpu.VMEM((r_rows, NB), BF),
            pltpu.VMEM((8, 4, 32, r_rows), BF),
            pltpu.VMEM((r_rows, s_rows), BF),
            pltpu.SemaphoreType.DMA((len(pieces),)),
            pltpu.SemaphoreType.DMA((2 * len(chunks),)),
        ],
        compiler_params=pltpu.CompilerParams(vmem_limit_bytes=32 * MIB),
        cost_estimate=pl.CostEstimate(
            flops=6 * s_rows * r_rows * NB, bytes_accessed=12 * MIB, transcendentals=0
        ),
        name="main",
    )(*chunks, *pieces)


def gather_green_x(v):
    xm, xp = shift(v, "x", 1), shift(v, "x", -1)
    far = jnp.stack([shift(xm[0], "x", 1), shift(xp[1], "x", -1)])
    return [v, xm, xp, far]


def both_cores(parts):
    return parts + [shift(v, "core", 1) for v in parts]


S_RING = (0, 3, 1, 2, 2)


def gather_points_x(b):
    half = DEV_ROWS // 2
    part = lax.dynamic_slice_in_dim(b, lax.axis_index("tm") * half, half, 0)
    xm, xp, far = shift(b, "x", 1), shift(b, "x", -1), shift(part, "x", 2)
    return [b, xm, xp, far, shift(far, "tm", 1)]


def gather_points_yz(b):
    far = shift(b, "y", 2)
    pair = jnp.concatenate([b, far_z(b)])
    ym, yp = shift(pair, "y", 1), shift(pair, "y", -1)
    zfar = far_z(far)
    return [pair, far, ym, zfar, yp]


def gather_green_yz(g):
    zh, y = lax.axis_index("zh"), lax.axis_index("y")
    gz = shift(g, "zh", 1)
    first = zh == 0
    pair = jnp.stack([jnp.where(first, g, gz), jnp.where(first, gz, g)], axis=1)
    parts = [pair, shift(pair, "y", -1), shift(pair, "y", 2), shift(pair, "y", 1)]
    out = jnp.zeros((2, 2, 4, 16, NB), BF)
    for k, v in enumerate(parts):
        out = lax.dynamic_update_slice_in_dim(out, v[:, :, None], lax.rem(y + k, 4), 2)
    return out.reshape(2, 8, 16, NB)


def project(green, s_block):
    rows = nt(green.reshape(-1, NB), s_block).astype(BF)
    return rows.reshape(*green.shape[:-1], s_block.shape[0])


def sum_over_x(parts):
    back = parts[0].astype(F32)
    for k in (2, 1, 3):
        back = back + shift(parts[k], "x", k).astype(F32)
    return back.astype(BF).reshape(256, -1)


def reduce_out(coef, time_weights):
    zh, y, core = (lax.axis_index(a) for a in ("zh", "y", "core"))
    tm = lax.axis_index("tm")
    coef = coef.reshape(8, 2, 16, NB)

    def for_core(k):
        return lax.dynamic_index_in_dim(coef, k, 1, keepdims=False)

    coef = for_core(core) + shift(for_core(1 - core), "core", 1)
    coef = coef.reshape(2, 4, 16, NB)

    def for_y(k):
        return lax.dynamic_index_in_dim(coef, lax.rem(y + k, 4), 1, keepdims=False)

    col = for_y(0)
    for k in (2, 1, 3):
        col = col + shift(for_y(k), "y", k)

    def weighted(f, z):
        w = lax.dynamic_slice(time_weights, (f, tm), (1, 1)) * (1.0 / NR)
        return w * lax.dynamic_index_in_dim(col, z, 0, keepdims=False)

    out = weighted(tm, zh)
    out = out + shift(weighted(1 - tm, zh), "tm", 1)
    out = out + shift(weighted(tm, 1 - zh), "zh", 1)
    out = out + far_z(weighted(1 - tm, 1 - zh))
    return out[None]


def shards(occupied_green, empty_green, basis, time_weights):
    lowest = jnp.array(-jnp.inf, BF)
    none, both = (0, 0, 0), (0, 1, 0)
    green = jnp.maximum(
        lax.pad(occupied_green, lowest, (both, none, none)),
        lax.pad(empty_green, lowest, ((1, 0, 0), none, none)),
    )
    green = gather_green_yz(green)
    s_pieces = gather_points_x(basis)
    s_block = assemble(s_pieces)
    r_pieces = both_cores(gather_points_yz(basis))
    greens = both_cores(gather_green_x(green))
    chunks = []
    for v in greens:
        chunks.append(project(v, s_block))
    parts = main(chunks, r_pieces, s_block.shape[0])
    coef = jnp.dot(sum_over_x(parts), s_block, preferred_element_type=F32)
    return reduce_out(coef, time_weights)


def solution(mesh):
    split = Mesh(
        mesh.devices.reshape(mesh.shape["tm"], 2, 4, 4, 2),
        ("tm", "zh", "y", "x", "core"),
    )
    in_specs = (P("tm", GRID, None), P("tm", GRID, None), P(GRID, None), P())
    out_specs = P("tm", GRID, None)

    return jax.shard_map(
        shards, mesh=split, in_specs=in_specs, out_specs=out_specs, check_vma=False
    )
```
